32 devices in a mesh: row: 8 (over y, x, core), col: 4 (over z).
Axes of the slice: x: 2, y: 2, z: 4, core: 2. Of those that a mesh axis runs over, the one named last changes fastest.
Arguments:
- features: bfloat16 [65536, 256], P(('row', 'col')), may hold values from -6 to 6
- tiles: bfloat16 [8, 4, 768, 128, 128], P('row', 'col'), as said below
- tile_rows: int32 [8, 4, 768], P('row', 'col'), may hold values from 0 to 63
- tile_cols: int32 [8, 4, 768], P('row', 'col'), may hold values from 0 to 127
- valid: int32 [8, 4, 768], P('row', 'col'), may hold values from 0 to 1, as said below
- weight: bfloat16 [256, 256], replicated, may hold values from -0.375 to 0.375
- bias: float32 [256], replicated, may hold values from -3 to 3
Outputs:
- hidden: bfloat16 [65536, 256], P(('row', 'col'))
The draws below stay inside these ranges and needn't reach their ends.
Inputs may be any that keep to these rules, and one draw needn't show every extreme that they name: Each cell holds between 96 and 384 valid slots at any positions; in every draw some cell has exactly 384 valid slots. `tiles`: tile entries are non-negative.
All inputs are finite; a program needn't handle non-finite values.
Results may differ from the reference program's by a relative error of at most 0.0039.
Values may be sent and summed in bfloat16 or wider, within the bound.
No kernel may reach another device: no remote copies, remote signals or barrier semaphores. Data moves between devices by JAX's collectives and lax.ppermute only.
A program may use at most 256 MiB of HBM per device.

```python
import jax
import jax.numpy as jnp
from jax import lax

F = 256
TILE = 128
SUB = 2048
TPD = 768
NODES = 65536
N_ROW = 8
N_COL = 4


def draw_tiles(key, part):
    shape = (N_ROW, N_COL, TPD, TILE, TILE)
    spread = (SUB / (TPD * TILE * TILE)) ** 0.5
    values = jnp.minimum(jnp.abs(jax.random.normal(key, shape, jnp.float32)) * spread, 5.0 * spread)
    return values.astype(jnp.bfloat16)


def draw_valid(key, part):
    subkeys = jax.random.split(key, 3)
    cells = N_ROW * N_COL
    shifts = jax.random.randint(subkeys[0], (cells,), 1, 4)
    counts = jnp.right_shift(jnp.full((cells,), TPD, jnp.int32), shifts)
    chosen = jax.random.randint(subkeys[1], (), 0, cells)
    counts = jnp.where(jnp.arange(cells) == chosen, TPD // 2, counts)
    orders = jax.vmap(lambda sub_key: jax.random.permutation(sub_key, TPD))(jax.random.split(subkeys[2], cells))
    valid_flags = (orders < counts[:, None]).astype(jnp.int32)
    return valid_flags.reshape(N_ROW, N_COL, TPD)


def touch_ends(values, own_key, smallest, high):
    shape = values.shape
    index_at = [jax.random.randint(jax.random.fold_in(own_key, axis), (), 0, shape[axis]) for axis in range(len(shape))]
    values = values.at[tuple(index_at)].set(smallest)
    longest = shape.index(max(shape))
    index_at[longest] = (index_at[longest] + 1) % shape[longest]
    return values.at[tuple(index_at)].set(high)


def block_scale(rng, dims, cuts, least, high):
    factor_of, own = 1.0, jax.random.fold_in(rng, 6)
    for dim, shards_of in cuts:
        heights = jnp.exp(jax.random.uniform(jax.random.fold_in(own, dim), (shards_of,), jnp.float32, least / len(cuts), high / len(cuts)))
        factor_of = factor_of * jnp.repeat(heights, dims[dim] // shards_of).reshape([-1 if axis == dim else 1 for axis in range(len(dims))])
    return factor_of


def gaussian(key, extent, scale, limit, pieces=(), kind=jnp.bfloat16):
    entries = jax.random.normal(key, extent, jnp.float32) * scale
    if len(pieces) > 0:
        entries = block_scale(key, extent, pieces, -0.22, 0.18) * entries
    return jnp.clip(entries, min=-limit, max=limit).astype(kind)


def setup_inputs(seed: int = 0) -> dict:
    key_list = jax.random.split(jax.random.key(seed), 8)
    features = gaussian(key_list[0], (NODES, F), 1.0, 6.0, ((0, 32),))
    tiles = draw_tiles(jax.random.fold_in(key_list[7], 71), 0)
    tile_rows = touch_ends(jax.random.randint(key_list[2], (N_ROW, N_COL, TPD), 0, SUB * N_COL // TILE), jax.random.fold_in(key_list[2], 1), 0, (SUB * N_COL // TILE) - 1).astype(jnp.int32)
    tile_cols = touch_ends(jax.random.randint(key_list[3], (N_ROW, N_COL, TPD), 0, SUB * N_ROW // TILE), jax.random.fold_in(key_list[3], 1), 0, (SUB * N_ROW // TILE) - 1).astype(jnp.int32)
    valid = draw_valid(jax.random.fold_in(key_list[7], 71), 0)
    weight = gaussian(key_list[5], (F, F), F ** -0.5, 0.375)
    bias = gaussian(key_list[6], (F,), 0.5, 3.0, (), jnp.float32)
    return {"features": features, "tiles": tiles, "tile_rows": tile_rows, "tile_cols": tile_cols, "valid": valid, "weight": weight, "bias": bias}


def reference(features, tiles, tile_rows, tile_cols, valid, weight, bias):
    row_tiles = SUB * N_COL // TILE
    grouped = features.reshape(N_ROW, N_COL, SUB, F)
    flat_tiles = tiles.reshape(N_ROW * N_COL, TPD, TILE, TILE)
    flat_rows = tile_rows.reshape(N_ROW * N_COL, TPD)
    flat_cols = tile_cols.reshape(N_ROW * N_COL, TPD)
    flat_valid = valid.reshape(N_ROW * N_COL, TPD)

    def one_cell(device):
        column = device % N_COL
        panel = jnp.take(grouped, column, axis=1).reshape(-1, TILE, F)
        chosen = panel[flat_cols[device]]
        products = jnp.einsum("bij,bjf->bif", flat_tiles[device].astype(jnp.float32), chosen.astype(jnp.float32))
        products = products * flat_valid[device].astype(jnp.float32)[:, None, None]
        partial_sum = jnp.zeros((row_tiles, TILE, F), jnp.float32)
        return partial_sum.at[flat_rows[device]].add(products)

    partials = lax.map(one_cell, jnp.arange(N_ROW * N_COL, dtype=jnp.int32))
    totals = jnp.sum(partials.reshape(N_ROW, N_COL, row_tiles, TILE, F), axis=1)
    aggregated = totals.reshape(N_ROW * N_COL * SUB, F).astype(jnp.bfloat16)
    mixed = jnp.dot(aggregated, weight, preferred_element_type=jnp.float32) + bias
    return jnp.maximum(mixed, 0.0).astype(jnp.bfloat16)
```

```python
import functools

import jax
import jax.numpy as jnp
from jax import lax
from jax.experimental import pallas as pl
from jax.experimental.pallas import tpu as pltpu
from jax.sharding import PartitionSpec as P


LANES = 128
GROUP = 4
UNROLL = 4
STAGES = 4
BATCH = GROUP * UNROLL


def plan_groups(cell_rows, cell_cols, cell_valid, row_tiles, col_tiles):
    slots = cell_rows.shape[0]
    live = cell_valid > 0
    row_ids = jnp.arange(row_tiles, dtype=jnp.int32)
    slot_ids = jnp.arange(slots, dtype=jnp.int32)
    hits = (cell_rows[:, None] == row_ids[None, :]) & live[:, None]
    counts = jnp.sum(hits.astype(jnp.int32), axis=0)
    groups = (counts + (GROUP - 1)) // GROUP
    total = jnp.sum(groups)
    before = jnp.sum(jnp.where(row_ids[None, :] < cell_rows[:, None], groups[None, :], 0), axis=1)
    same = (cell_rows[:, None] == cell_rows[None, :]) & live[None, :] & (slot_ids[None, :] < slot_ids[:, None])
    rank = jnp.sum(same.astype(jnp.int32), axis=1)
    place = jnp.where(live, before * GROUP + rank, -1)
    room = -(-(slots + row_tiles * (GROUP - 1)) // BATCH) * BATCH
    seats = jnp.arange(room, dtype=jnp.int32)
    code = slot_ids * col_tiles + cell_cols + 1
    entries = jnp.sum(jnp.where(seats[:, None] == place[None, :], code[None, :], 0), axis=1) - 1
    ends = jnp.sum(jnp.where(row_ids[:, None] >= row_ids[None, :], groups[None, :], 0), axis=1)
    group_ids = jnp.arange(room // GROUP, dtype=jnp.int32)
    group_rows = jnp.sum((ends[None, :] <= group_ids[:, None]).astype(jnp.int32), axis=1)
    group_rows = jnp.minimum(group_rows, row_tiles - 1)
    turns = (total + (UNROLL - 1)) // UNROLL
    return entries, group_rows, turns.reshape(1)


def tile_kernel(entries, group_rows, turns, place, *refs, parts, col_tiles):
    blocks = refs[:parts]
    tiles, sums, panel, ring, tile_sems, block_sems = refs[parts:]
    tile_size = ring.shape[1]
    block_tiles = panel.shape[0] // parts
    count = turns[0]
    zero_seat = STAGES * BATCH

    def fetch(turn):
        stage = lax.rem(turn, STAGES)
        for seat in range(BATCH):
            slot = jnp.maximum(entries[turn * BATCH + seat], 0) // col_tiles
            pltpu.make_async_copy(tiles.at[slot], ring.at[stage * BATCH + seat], tile_sems.at[stage]).start()

    def block_copy(part):
        return pltpu.make_async_copy(
            blocks[part], panel.at[pl.ds(place[part] * block_tiles, block_tiles)], block_sems.at[part]
        )

    for part in range(parts):
        block_copy(part).start()
    for turn in range(STAGES):
        pl.when(turn < count)(functools.partial(fetch, turn))
    ring[zero_seat] = jnp.zeros(ring.shape[1:], ring.dtype)
    sums[...] = jnp.zeros(sums.shape, sums.dtype)
    for part in range(parts):
        block_copy(part).wait()

    def step(turn, carry):
        stage = lax.rem(turn, STAGES)
        base = stage * BATCH
        pltpu.make_async_copy(
            tiles.at[pl.ds(0, BATCH)], ring.at[pl.ds(base, BATCH)], tile_sems.at[stage]
        ).wait()
        products = []
        for group in range(UNROLL):
            left, right = [], []
            for member in range(GROUP):
                seat = group * GROUP + member
                entry = entries[turn * BATCH + seat]
                left.append(ring[jnp.where(entry < 0, zero_seat, base + seat)])
                right.append(panel[lax.rem(jnp.maximum(entry, 0), col_tiles)])
            products.append(
                jnp.dot(
                    jnp.concatenate(left, axis=1),
                    jnp.concatenate(right, axis=0),
                    preferred_element_type=jnp.float32,
                )
            )
        for group in range(UNROLL):
            row = group_rows[turn * UNROLL + group]
            sums[row] += products[group]
        pl.when(turn + STAGES < count)(lambda: fetch(turn + STAGES))
        return carry

    lax.fori_loop(0, count, step, 0)


def tile_products(plan, place, blocks, cell_tiles, row_tiles, col_tiles):
    entries, group_rows, turns = plan
    parts = len(blocks)
    slots, tile_size, _ = cell_tiles.shape
    lanes = blocks[0].shape[-1]
    blocks = [block.reshape(-1, tile_size, lanes) for block in blocks]
    block_tiles = blocks[0].shape[0]
    smem = pl.BlockSpec(memory_space=pltpu.SMEM)
    hbm = pl.BlockSpec(memory_space=pltpu.HBM)
    return pl.pallas_call(
        functools.partial(tile_kernel, parts=parts, col_tiles=col_tiles),
        out_shape=jax.ShapeDtypeStruct((row_tiles, tile_size, lanes), jnp.float32),
        in_specs=[smem] * 4 + [hbm] * (parts + 1),
        out_specs=pl.BlockSpec(memory_space=pltpu.VMEM),
        scratch_shapes=[
            pltpu.VMEM((parts * block_tiles, tile_size, lanes), jnp.bfloat16),
            pltpu.VMEM((STAGES * BATCH + 1, tile_size, tile_size), jnp.bfloat16),
            pltpu.SemaphoreType.DMA((STAGES,)),
            pltpu.SemaphoreType.DMA((parts,)),
        ],
        cost_estimate=pl.CostEstimate(
            flops=slots * tile_size * tile_size * lanes,
            bytes_accessed=slots * tile_size * tile_size + row_tiles * tile_size * lanes * 4,
            transcendentals=0,
        ),
        name="tile_products",
    )(entries, group_rows, turns, place, *blocks, cell_tiles)


def swap(value, axis, bits):
    size = lax.axis_size(axis)
    return lax.ppermute(value, axis, [(i, i ^ bits) for i in range(size)])


def gather_row(piece):
    size = lax.axis_size("row")
    if size & (size - 1):
        whole = lax.all_gather(piece, "row", axis=0)
        own = lax.axis_index("row")
        order = [lax.rem(own + k, size) for k in range(size)]
        return [lax.dynamic_index_in_dim(whole, k, 0, keepdims=False) for k in order], order
    far = {bits: swap(piece, "row", bits) for bits in range(2, size, 2)}
    far[0] = piece
    pieces = dict(far)
    for bits, value in far.items():
        if size > 1:
            pieces[bits | 1] = swap(value, "row", bits ^ 1 if bits == 0 else 1)
    own = lax.axis_index("row")
    return [pieces[b] for b in range(size)], [own ^ b for b in range(size)]


def reduce_col(partial_rows, out_rows):
    size = lax.axis_size("col")
    own = lax.axis_index("col")

    def block(index):
        return lax.dynamic_slice_in_dim(partial_rows, jnp.clip(index, 0, size - 1) * out_rows, out_rows)

    up = down = None
    for turn in range(size - 1):
        send_up = block(size - 1 - turn + own)
        send_down = block(turn - (size - 1 - own))
        if turn > 0:
            send_up = send_up + up.astype(jnp.float32)
            send_down = send_down + down.astype(jnp.float32)
        up = lax.ppermute(send_up.astype(jnp.bfloat16), "col", [(i, i + 1) for i in range(min(turn + 1, size - 1))])
        down = lax.ppermute(
            send_down.astype(jnp.bfloat16), "col", [(size - 1 - i, size - 2 - i) for i in range(min(turn + 1, size - 1))]
        )
    total = block(own)
    if size > 1:
        total = total + up.astype(jnp.float32) + down.astype(jnp.float32)
    return total


def on_device(features, tiles, tile_rows, tile_cols, valid, weight, bias):
    sub_rows, width = features.shape
    tile_size = tiles.shape[3]
    row_count = lax.axis_size("row")
    col_count = lax.axis_size("col")
    row_tiles = sub_rows * col_count // tile_size
    col_tiles = sub_rows * row_count // tile_size
    plan = plan_groups(tile_rows[0, 0], tile_cols[0, 0], valid[0, 0], row_tiles, col_tiles)
    lanes = LANES if width % LANES == 0 else width
    mixed = bias[None, :]
    anchor = None
    for start in range(0, width, lanes):
        piece = features[:, start : start + lanes]
        if anchor is not None:
            piece, anchor = lax.optimization_barrier((piece, anchor))
        blocks, order = gather_row(piece)
        anchor = blocks[-2] if len(blocks) > 1 else blocks[-1]
        place = jnp.stack(order).astype(jnp.int32)
        sums = tile_products(plan, place, blocks, tiles[0, 0], row_tiles, col_tiles)
        total = reduce_col(sums.reshape(row_tiles * tile_size, lanes), sub_rows)
        aggregated = total.astype(jnp.bfloat16)
        mixed = mixed + jnp.dot(aggregated, weight[start : start + lanes], preferred_element_type=jnp.float32)
    return jnp.maximum(mixed, 0.0).astype(jnp.bfloat16)


def solution(mesh):
    return jax.shard_map(
        on_device,
        mesh=mesh,
        in_specs=(
            P(("row", "col"), None),
            P("row", "col", None, None, None),
            P("row", "col", None),
            P("row", "col", None),
            P("row", "col", None),
            P(),
            P(),
        ),
        out_specs=P(("row", "col"), None),
        check_vma=False,
    )
```

```python
import functools

import jax
import jax.numpy as jnp
from jax import lax
from jax.experimental import pallas as pl
from jax.experimental.pallas import tpu as pltpu
from jax.sharding import PartitionSpec as P


LANES = 128
GROUP = 2
UNROLL = 16
STAGES = 4
BATCH = GROUP * UNROLL


def channel_chunks(width):
    lanes = LANES if width % LANES == 0 else width
    return [(start, lanes) for start in range(0, width, lanes)]


def plan_groups(cell_rows, cell_cols, cell_valid, row_tiles, col_bits):
    slots = cell_rows.shape[0]
    live = cell_valid > 0
    row_ids = jnp.arange(row_tiles, dtype=jnp.int32)
    slot_ids = jnp.arange(slots, dtype=jnp.int32)
    hits = (cell_rows[:, None] == row_ids[None, :]) & live[:, None]
    counts = jnp.sum(hits.astype(jnp.int32), axis=0)
    groups = (counts + (GROUP - 1)) // GROUP
    total = jnp.sum(groups)
    before = jnp.sum(jnp.where(row_ids[None, :] < cell_rows[:, None], groups[None, :], 0), axis=1)
    same = (cell_rows[:, None] == cell_rows[None, :]) & live[None, :] & (slot_ids[None, :] < slot_ids[:, None])
    rank = jnp.sum(same.astype(jnp.int32), axis=1)
    place = jnp.where(live, before * GROUP + rank, -1)
    room = -(-(slots + row_tiles * (GROUP - 1)) // BATCH) * BATCH
    seats = jnp.arange(room, dtype=jnp.int32)
    code = slot_ids * (1 << col_bits) + cell_cols + 1
    entries = jnp.sum(jnp.where(seats[:, None] == place[None, :], code[None, :], 0), axis=1) - 1
    ends = jnp.sum(jnp.where(row_ids[:, None] >= row_ids[None, :], groups[None, :], 0), axis=1)
    group_ids = jnp.arange(room // GROUP, dtype=jnp.int32)
    group_rows = jnp.sum((ends[None, :] <= group_ids[:, None]).astype(jnp.int32), axis=1)
    group_rows = jnp.minimum(group_rows, row_tiles - 1)
    turns = (total + (UNROLL - 1)) // UNROLL
    return entries, group_rows, turns.reshape(1)


def tile_kernel(entries, group_rows, turns, place, picks, *refs, parts, col_bits, narrow, wide):
    blocks = refs[:parts]
    tiles = refs[parts]
    outs = refs[parts + 1 : parts + 1 + narrow + wide]
    sums, panel, ring, tile_sems = refs[parts + 1 + narrow + wide :]
    block_tiles = panel.shape[0] // parts
    count = turns[0]
    zero_seat = STAGES * BATCH

    def fetch(turn, seats=range(BATCH)):
        stage = lax.rem(turn, STAGES)
        for seat in seats:
            slot = lax.shift_right_logical(jnp.maximum(entries[turn * BATCH + seat], 0), col_bits)
            pltpu.make_async_copy(tiles.at[slot], ring.at[stage * BATCH + seat], tile_sems.at[stage]).start()

    def arrive(turn):
        stage = lax.rem(turn, STAGES)
        pltpu.make_async_copy(
            tiles.at[pl.ds(0, BATCH)], ring.at[pl.ds(stage * BATCH, BATCH)], tile_sems.at[stage]
        ).wait()

    lax.fori_loop(0, jnp.minimum(count, STAGES - 1), lambda turn, carry: fetch(turn) or carry, 0)
    ring[zero_seat] = jnp.zeros(ring.shape[1:], ring.dtype)
    sums[...] = jnp.zeros(sums.shape, sums.dtype)
    for part in range(parts):
        panel[pl.ds(place[part] * block_tiles, block_tiles)] = blocks[part][...]

    def step(ahead, turn, carry):
        base = lax.rem(turn, STAGES) * BATCH
        arrive(turn)
        products = []
        for group in range(UNROLL):
            if ahead:
                fetch(turn + ahead, range(group * GROUP, (group + 1) * GROUP))
            left, right = [], []
            for member in range(GROUP):
                seat = group * GROUP + member
                entry = entries[turn * BATCH + seat]
                left.append(ring[jnp.where(entry < 0, zero_seat, base + seat)])
                right.append(panel[jnp.maximum(entry, 0) & ((1 << col_bits) - 1)])
            products.append(
                jnp.dot(
                    jnp.concatenate(left, axis=1),
                    jnp.concatenate(right, axis=0),
                    preferred_element_type=jnp.float32,
                )
            )
        for group in range(UNROLL):
            sums[group_rows[turn * UNROLL + group]] += products[group]
        return carry

    steady = jnp.maximum(count - (STAGES - 1), 0)
    lax.fori_loop(0, steady, functools.partial(step, STAGES - 1), 0)
    lax.fori_loop(steady, count, functools.partial(step, 0), 0)

    for number, out in enumerate(outs):
        base = picks[number] * block_tiles

        def emit(tile, carry):
            out[tile] = sums[base + tile].astype(out.dtype)
            return carry

        lax.fori_loop(0, block_tiles, emit, 0, unroll=4)


def tile_products(plan, place, picks, narrow, wide, blocks, cell_tiles, row_tiles, col_bits):
    entries, group_rows, turns = plan
    parts = len(blocks)
    slots, tile_size, _ = cell_tiles.shape
    lanes = blocks[0].shape[-1]
    blocks = [block.reshape(-1, tile_size, lanes) for block in blocks]
    block_tiles = blocks[0].shape[0]
    smem = pl.BlockSpec(memory_space=pltpu.SMEM)
    vmem = pl.BlockSpec(memory_space=pltpu.VMEM)
    hbm = pl.BlockSpec(memory_space=pltpu.HBM)
    shape = (block_tiles, tile_size, lanes)
    outs = pl.pallas_call(
        functools.partial(tile_kernel, parts=parts, col_bits=col_bits, narrow=narrow, wide=wide),
        out_shape=[jax.ShapeDtypeStruct(shape, jnp.bfloat16)] * narrow
        + [jax.ShapeDtypeStruct(shape, jnp.float32)] * wide,
        in_specs=[smem] * 5 + [vmem] * parts + [hbm],
        out_specs=[vmem] * (narrow + wide),
        scratch_shapes=[
            pltpu.VMEM((row_tiles, tile_size, lanes), jnp.float32),
            pltpu.VMEM((parts * block_tiles, tile_size, lanes), jnp.bfloat16),
            pltpu.VMEM((STAGES * BATCH + 1, tile_size, tile_size), jnp.bfloat16),
            pltpu.SemaphoreType.DMA((STAGES,)),
        ],
        cost_estimate=pl.CostEstimate(
            flops=slots * tile_size * tile_size * lanes,
            bytes_accessed=slots * tile_size * tile_size + row_tiles * tile_size * lanes,
            transcendentals=0,
        ),
        name="tile_products",
    )(entries, group_rows, turns, place, picks, *blocks, cell_tiles)
    return [out.reshape(block_tiles * tile_size, lanes) for out in outs]


def swap(value, bits):
    size = lax.axis_size("row")
    return lax.ppermute(value, "row", [(i, i ^ bits) for i in range(size)])


def gather_far(piece):
    size = lax.axis_size("row")
    if size & (size - 1):
        far = {0: piece}
        for k in range(1, size):
            far[k] = lax.ppermute(piece, "row", [(i, (i - k) % size) for i in range(size)])
        return far
    return {bits: swap(piece, bits) if bits else piece for bits in range(0, size, 2)}


def gather_near(far):
    size = lax.axis_size("row")
    pieces = dict(far)
    if size > 1 and size & (size - 1) == 0:
        for bits, value in far.items():
            pieces[bits | 1] = swap(value, 1)
    return [pieces[k] for k in range(size)]


def gather_order():
    size = lax.axis_size("row")
    own = lax.axis_index("row")
    offsets = lax.broadcasted_iota(jnp.int32, (size,), 0)
    return lax.rem(own + offsets, size) if size & (size - 1) else own ^ offsets


def disjoint(pairs):
    return len({s for s, _ in pairs}) == len(pairs) and len({t for _, t in pairs}) == len(pairs)


def both_ways(ahead, up_pairs):
    size = lax.axis_size("col")
    own = lax.axis_index("col")
    down_pairs = [(size - 1 - s, size - 1 - t) for s, t in up_pairs]
    if disjoint(up_pairs + down_pairs):
        going_up = functools.reduce(jnp.logical_or, [own == s for s, _ in up_pairs])
        return [(jnp.where(going_up, own + ahead, own - ahead), up_pairs + down_pairs)]
    return [(own + ahead, up_pairs), (own - ahead, down_pairs)]


def line_messages():
    size = lax.axis_size("col")
    inner = size - 2
    hops = [both_ways(inner + 1 - turn, [(i, i + 1) for i in range(turn + 1)]) for turn in range(inner - 1)]
    near = []
    if size > 1:
        own = lax.axis_index("col")
        near = [(own + 1, [(i, i + 1) for i in range(size - 1)]), (own - 1, [(i + 1, i) for i in range(size - 1)])]
    far = both_ways(2, [(i, i + 2) for i in range(size - 2)]) if size > 2 else []
    return hops, near, far


def line_picks():
    hops, near, far = line_messages()
    first = hops[0] if hops else far
    later = [message for turn in hops[1:] for message in turn] + (far if hops else [])
    narrow = [index for index, _ in first + near]
    wide = [index for index, _ in later] + [lax.axis_index("col")]
    last = lax.axis_size("col") - 1
    numbers = lax.broadcasted_iota(jnp.int32, (len(narrow + wide),), 0)
    picks = jnp.zeros_like(numbers)
    for number, index in enumerate(narrow + wide):
        picks = jnp.where(numbers == number, jnp.clip(index, 0, last), picks)
    return picks, len(narrow), len(wide)


def reduce_line(picked):
    hops, near, far = line_messages()
    first = len(hops[0] if hops else far)
    sent = picked[:first]
    near_sent = picked[first : first + len(near)]
    later = list(picked[first + len(near) :])

    def move(values, messages):
        return [lax.ppermute(value, "col", pairs) for value, (_, pairs) in zip(values, messages)]

    def added(messages, carried):
        values = [later.pop(0) for _ in messages]
        carried = carried * (len(values) if len(carried) < len(values) else 1)
        if len(values) < len(carried):
            carried = carried[:1]
        return [(v + c.astype(jnp.float32)).astype(jnp.bfloat16) for v, c in zip(values, carried)]

    carried = None
    for turn in hops:
        values = sent if carried is None else added(turn, carried)
        carried = move(values, turn)
    parts = move(near_sent, near)
    if far:
        values = sent if carried is None else added(far, carried)
        parts = parts + move(values, far)
    return later[0], parts


def add_parts(own, parts):
    for part in parts:
        own = own + part.astype(jnp.float32)
    return own.astype(jnp.bfloat16)


def on_device(features, tiles, tile_rows, tile_cols, valid, weight, bias):
    sub_rows, width = features.shape
    tile_size = tiles.shape[3]
    row_tiles = sub_rows * lax.axis_size("col") // tile_size
    col_tiles = sub_rows * lax.axis_size("row") // tile_size
    col_bits = (col_tiles - 1).bit_length()
    chunks = channel_chunks(width)
    plan = plan_groups(tile_rows[0, 0], tile_cols[0, 0], valid[0, 0], row_tiles, col_bits)
    picks, narrow, wide = line_picks()
    place = gather_order()
    far = []
    for start, size in chunks:
        piece = features[:, start : start + size]
        if far:
            piece, far[-1] = lax.optimization_barrier((piece, far[-1]))
        far.append(gather_far(piece))
    mixed = bias[None, :]
    for index, (start, size) in enumerate(chunks):
        blocks = gather_near(far[index])
        picked = tile_products(plan, place, picks, narrow, wide, blocks, tiles[0, 0], row_tiles, col_bits)
        own, parts = reduce_line(picked)
        aggregated = add_parts(own, parts)
        mixed = mixed + jnp.dot(aggregated, weight[start : start + size], preferred_element_type=jnp.float32)
        if index < len(chunks) - 1:
            mixed = lax.optimization_barrier(mixed)
    return jnp.maximum(mixed, 0.0).astype(jnp.bfloat16)


def solution(mesh):
    def call(features, *operands):
        step = jax.shard_map(
            on_device,
            mesh=mesh,
            in_specs=(
                P(("row", "col"), None),
                P("row", "col", None, None, None),
                P("row", "col", None),
                P("row", "col", None),
                P("row", "col", None),
                P(),
                P(),
            ),
            out_specs=P(("row", "col"), None),
            check_vma=False,
        )
        return step(features, *operands)

    return call
```

```python
import functools

import jax
import jax.numpy as jnp
from jax import lax
from jax.experimental import pallas as pl
from jax.experimental.pallas import tpu as pltpu
from jax.sharding import PartitionSpec as P


LANES = 128
GROUP = 2
UNROLL = 16
STAGES = 4
VMEM_LIMIT = 44 * 1024 * 1024
KEPT_ROOM = 6
BATCH = GROUP * UNROLL


def channel_chunks(width):
    lanes = LANES if width % LANES == 0 else width
    return [(start, lanes) for start in range(0, width, lanes)]


def plan_groups(cell_rows, cell_cols, live, row_tiles, col_bits):
    slots = cell_rows.shape[0]
    row_ids = jnp.arange(row_tiles, dtype=jnp.int32)
    slot_ids = jnp.arange(slots, dtype=jnp.int32)
    hits = (cell_rows[:, None] == row_ids[None, :]) & live[:, None]
    counts = jnp.sum(hits.astype(jnp.int32), axis=0)
    groups = (counts + (GROUP - 1)) // GROUP
    total = jnp.sum(groups)
    before = jnp.sum(jnp.where(row_ids[None, :] < cell_rows[:, None], groups[None, :], 0), axis=1)
    same = (cell_rows[:, None] == cell_rows[None, :]) & live[None, :] & (slot_ids[None, :] < slot_ids[:, None])
    rank = jnp.sum(same.astype(jnp.int32), axis=1)
    place = jnp.where(live, before * GROUP + rank, -1)
    room = -(-(slots + row_tiles * (GROUP - 1)) // BATCH) * BATCH
    seats = jnp.arange(room, dtype=jnp.int32)
    code = slot_ids * (1 << col_bits) + cell_cols + 1
    entries = jnp.sum(jnp.where(seats[:, None] == place[None, :], code[None, :], 0), axis=1) - 1
    ends = jnp.sum(jnp.where(row_ids[:, None] >= row_ids[None, :], groups[None, :], 0), axis=1)
    group_ids = jnp.arange(room // GROUP, dtype=jnp.int32)
    group_rows = jnp.sum((ends[None, :] <= group_ids[:, None]).astype(jnp.int32), axis=1)
    group_rows = jnp.minimum(group_rows, row_tiles - 1)
    turns = (total + (UNROLL - 1)) // UNROLL
    return entries, group_rows, turns.reshape(1)


def tile_kernel(*refs, lists, parts, begun, keep, col_bits, narrow, wide):
    plans = [refs[3 * k : 3 * k + 3] for k in range(lists)]
    place, picks = refs[3 * lists : 3 * lists + 2]
    refs = refs[3 * lists + 2 :]
    blocks = refs[: len(parts)]
    tiles = refs[len(parts)]
    started = refs[len(parts) + 1] if begun else None
    outs = refs[len(parts) + 1 + begun :][: narrow + wide + keep]
    sums, panel, ring, tile_sems, whole_sem, *earlier = refs[len(parts) + 1 + begun + narrow + wide + keep :]
    block_tiles = blocks[0].shape[0]
    zero_seat = STAGES * BATCH
    spare = place[parts[0]] * block_tiles

    def fetch(entries, turn, seats=range(BATCH)):
        stage = lax.rem(turn, STAGES)
        for seat in seats:
            slot = lax.shift_right_logical(jnp.maximum(entries[turn * BATCH + seat], 0), col_bits)
            pltpu.make_async_copy(tiles.at[slot], ring.at[stage * BATCH + seat], tile_sems.at[stage]).start()

    def first_fetches(entries, count):
        lax.fori_loop(0, jnp.minimum(count, STAGES - 1), lambda turn, carry: fetch(entries, turn) or carry, 0)

    def step(ahead, entries, group_rows, turn, carry):
        stage = lax.rem(turn, STAGES)
        base = stage * BATCH
        pltpu.make_async_copy(
            tiles.at[pl.ds(0, BATCH)], ring.at[pl.ds(base, BATCH)], tile_sems.at[stage]
        ).wait()
        products = []
        for group in range(UNROLL):
            if ahead:
                fetch(entries, turn + ahead, range(group * GROUP, (group + 1) * GROUP))
            left, right = [], []
            for member in range(GROUP):
                seat = group * GROUP + member
                entry = entries[turn * BATCH + seat]
                left.append(ring[jnp.where(entry < 0, zero_seat, base + seat)])
                right.append(panel[jnp.where(entry < 0, spare, entry & ((1 << col_bits) - 1))])
            products.append(
                jnp.dot(
                    jnp.concatenate(left, axis=1),
                    jnp.concatenate(right, axis=0),
                    preferred_element_type=jnp.float32,
                )
            )
        for group in range(UNROLL):
            sums[group_rows[turn * UNROLL + group]] += products[group]
        return carry

    first_fetches(plans[0][0], plans[0][2][0])
    ring[zero_seat] = jnp.zeros(ring.shape[1:], ring.dtype)
    if begun:
        restore = pltpu.make_async_copy(started.at[pl.ds(0, sums.shape[0])], earlier[0], whole_sem)
        restore.start()
    sums[...] = jnp.zeros(sums.shape, sums.dtype)
    for number, part in enumerate(parts):
        panel[pl.ds(place[part] * block_tiles, block_tiles)] = blocks[number][...]
    for number, (entries, group_rows, turns) in enumerate(plans):
        count = turns[0]
        if number:
            first_fetches(entries, count)
        steady = jnp.maximum(count - (STAGES - 1), 0)
        lax.fori_loop(0, steady, functools.partial(step, STAGES - 1, entries, group_rows), 0)
        lax.fori_loop(steady, count, functools.partial(step, 0, entries, group_rows), 0)

    if keep:
        save = pltpu.make_async_copy(sums, outs[0].at[pl.ds(0, sums.shape[0])], whole_sem)
        save.start()
        save.wait()
        return
    if begun:
        restore.wait()
    for number, out in enumerate(outs):
        base = picks[number] * block_tiles

        def emit(tile, carry):
            value = sums[base + tile]
            if begun:
                value = value + earlier[0][base + tile]
            out[tile] = value.astype(out.dtype)
            return carry

        lax.fori_loop(0, block_tiles, emit, 0, unroll=4)


def tile_products(plans, place, picks, narrow, wide, blocks, cell_tiles, row_tiles, col_bits, begun=None, keep=False):
    parts = sorted(blocks)
    slots, tile_size, _ = cell_tiles.shape
    lanes = blocks[parts[0]].shape[-1]
    values = [blocks[part].reshape(-1, tile_size, lanes) for part in parts]
    block_tiles = values[0].shape[0]
    if keep:
        narrow = wide = 0
    smem = pl.BlockSpec(memory_space=pltpu.SMEM)
    vmem = pl.BlockSpec(memory_space=pltpu.VMEM)
    hbm = pl.BlockSpec(memory_space=pltpu.HBM)
    shape = (block_tiles, tile_size, lanes)
    total = jax.ShapeDtypeStruct((row_tiles, tile_size, lanes), jnp.float32)
    operands = [array for plan in plans for array in plan] + [place, picks] + values + [cell_tiles]
    in_specs = [smem] * (3 * len(plans) + 2) + [vmem] * len(values) + [hbm]
    if begun is not None:
        operands.append(begun)
        in_specs.append(hbm)
    sums = pltpu.VMEM(total.shape, total.dtype)
    scratch = [
        sums,
        pltpu.VMEM((1 << col_bits, tile_size, lanes), jnp.bfloat16),
        pltpu.VMEM((STAGES * BATCH + 1, tile_size, tile_size), jnp.bfloat16),
        pltpu.SemaphoreType.DMA((STAGES,)),
        pltpu.SemaphoreType.DMA(()),
    ] + [sums] * (begun is not None)
    outs = pl.pallas_call(
        functools.partial(
            tile_kernel,
            lists=len(plans),
            parts=parts,
            begun=int(begun is not None),
            keep=int(keep),
            col_bits=col_bits,
            narrow=narrow,
            wide=wide,
        ),
        out_shape=[jax.ShapeDtypeStruct(shape, jnp.bfloat16)] * narrow
        + [jax.ShapeDtypeStruct(shape, jnp.float32)] * wide
        + [jax.ShapeDtypeStruct((KEPT_ROOM * row_tiles, tile_size, lanes), jnp.float32)] * keep,
        in_specs=in_specs,
        out_specs=[hbm if keep else vmem] * (narrow + wide + keep),
        scratch_shapes=scratch,
        compiler_params=pltpu.CompilerParams(vmem_limit_bytes=VMEM_LIMIT),
        cost_estimate=pl.CostEstimate(
            flops=slots * tile_size * tile_size * lanes,
            bytes_accessed=slots * tile_size * tile_size + row_tiles * tile_size * lanes,
            transcendentals=0,
        ),
        name="tile_products",
    )(*operands)
    if keep:
        return outs[0]
    return [out.reshape(block_tiles * tile_size, lanes) for out in outs[: narrow + wide]]


def swap(value, bits):
    size = lax.axis_size("row")
    return lax.ppermute(value, "row", [(i, i ^ bits) for i in range(size)])


def late_offset():
    size = lax.axis_size("row")
    return size - 2 if size > 2 and size & (size - 1) == 0 else None


def gather_far(piece):
    size = lax.axis_size("row")
    far = {0: piece}
    if size & (size - 1):
        for k in range(1, size):
            far[k] = lax.ppermute(piece, "row", [(i, (i - k) % size) for i in range(size)])
        return far
    for bits in range(2, size, 2):
        far[bits] = swap(piece, bits)
    return far


def gather_near(far):
    size = lax.axis_size("row")
    pieces = dict(far)
    if size > 1 and size & (size - 1) == 0:
        for bits, value in far.items():
            pieces[bits | 1] = swap(value, 1)
    return pieces


def gather_order():
    size = lax.axis_size("row")
    own = lax.axis_index("row")
    offsets = lax.broadcasted_iota(jnp.int32, (size,), 0)
    return lax.rem(own + offsets, size) if size & (size - 1) else own ^ offsets


def disjoint(pairs):
    return len({s for s, _ in pairs}) == len(pairs) and len({t for _, t in pairs}) == len(pairs)


def both_ways(ahead, up_pairs):
    size = lax.axis_size("col")
    own = lax.axis_index("col")
    down_pairs = [(size - 1 - s, size - 1 - t) for s, t in up_pairs]
    if disjoint(up_pairs + down_pairs):
        going_up = functools.reduce(jnp.logical_or, [own == s for s, _ in up_pairs])
        return [(jnp.where(going_up, own + ahead, own - ahead), up_pairs + down_pairs)]
    return [(own + ahead, up_pairs), (own - ahead, down_pairs)]


def line_messages():
    size = lax.axis_size("col")
    inner = size - 2
    hops = [both_ways(inner + 1 - turn, [(i, i + 1) for i in range(turn + 1)]) for turn in range(inner - 1)]
    near = []
    if size > 1:
        own = lax.axis_index("col")
        near = [(own + 1, [(i, i + 1) for i in range(size - 1)]), (own - 1, [(i + 1, i) for i in range(size - 1)])]
    far = both_ways(2, [(i, i + 2) for i in range(size - 2)]) if size > 2 else []
    return hops, near, far


def line_picks():
    hops, near, far = line_messages()
    first = hops[0] if hops else far
    later = [message for turn in hops[1:] for message in turn] + (far if hops else [])
    narrow = [index for index, _ in first + near]
    wide = [index for index, _ in later] + [lax.axis_index("col")]
    last = lax.axis_size("col") - 1
    numbers = lax.broadcasted_iota(jnp.int32, (len(narrow + wide),), 0)
    picks = jnp.zeros_like(numbers)
    for number, index in enumerate(narrow + wide):
        picks = jnp.where(numbers == number, jnp.clip(index, 0, last), picks)
    return picks, len(narrow), len(wide)


def reduce_line(picked):
    hops, near, far = line_messages()
    first = len(hops[0] if hops else far)
    sent = picked[:first]
    near_sent = picked[first : first + len(near)]
    later = list(picked[first + len(near) :])

    def move(values, messages):
        return [lax.ppermute(value, "col", pairs) for value, (_, pairs) in zip(values, messages)]

    def added(messages, carried):
        values = [later.pop(0) for _ in messages]
        carried = carried * (len(values) if len(carried) < len(values) else 1)
        if len(values) < len(carried):
            carried = carried[:1]
        return [(v + c.astype(jnp.float32)).astype(jnp.bfloat16) for v, c in zip(values, carried)]

    carried = None
    for turn in hops:
        values = sent if carried is None else added(turn, carried)
        carried = move(values, turn)
    parts = move(near_sent, near)
    if far:
        values = sent if carried is None else added(far, carried)
        parts = parts + move(values, far)
    return later[0], parts


def add_parts(own, parts):
    for part in parts:
        own = own + part.astype(jnp.float32)
    return own.astype(jnp.bfloat16)


def on_device(features, tiles, tile_rows, tile_cols, valid, weight, bias):
    sub_rows, width = features.shape
    tile_size = tiles.shape[3]
    row_tiles = sub_rows * lax.axis_size("col") // tile_size
    col_tiles = sub_rows * lax.axis_size("row") // tile_size
    col_bits = (col_tiles - 1).bit_length()
    chunks = channel_chunks(width)
    late = late_offset()
    cell_rows, cell_cols, live = tile_rows[0, 0], tile_cols[0, 0], valid[0, 0] > 0
    picks, narrow, wide = line_picks()
    place = gather_order()
    lives = [live]
    if late is not None:
        offset = (cell_cols // (sub_rows // tile_size)) ^ lax.axis_index("row")
        after = (offset | 1) == (late | 1)
        lives = [live & ~after, live & after]
    plans = [plan_groups(cell_rows, cell_cols, part, row_tiles, col_bits) for part in lives]
    far = []
    for start, size in chunks:
        far.append(gather_far(features[:, start : start + size]))
    products = functools.partial(
        tile_products, cell_tiles=tiles[0, 0], row_tiles=row_tiles, col_bits=col_bits, place=place, picks=picks
    )
    mixed = bias[None, :]
    for index, (start, size) in enumerate(chunks):
        begun, used = None, plans
        if index == 0 and late is not None:
            blocks = gather_near({bits: far[0][bits] for bits in far[0] if bits != late})
            begun = products(plans[:1], narrow=narrow, wide=wide, blocks=blocks, keep=True)
            used = plans[1:]
            far[0] = {late: far[0][late]}
        blocks = gather_near(far[index])
        picked = products(used, narrow=narrow, wide=wide, blocks=blocks, begun=begun)
        own, parts = reduce_line(picked)
        aggregated = add_parts(own, parts)
        mixed = mixed + jnp.dot(aggregated, weight[start : start + size], preferred_element_type=jnp.float32)
        if index < len(chunks) - 1:
            mixed = lax.optimization_barrier(mixed)
    return jnp.maximum(mixed, 0.0).astype(jnp.bfloat16)


def solution(mesh):
    def call(features, *operands):
        step = jax.shard_map(
            on_device,
            mesh=mesh,
            in_specs=(
                P(("row", "col"), None),
                P("row", "col", None, None, None),
                P("row", "col", None),
                P("row", "col", None),
                P("row", "col", None),
                P(),
                P(),
            ),
            out_specs=P(("row", "col"), None),
            check_vma=False,
        )
        return step(features, *operands)

    return call
```

```python
import functools

import jax
import jax.numpy as jnp
from jax import lax
from jax.experimental import pallas as pl
from jax.experimental.pallas import tpu as pltpu
from jax.sharding import PartitionSpec as P


LANES = 128
GROUP = 2
UNROLL = 16
STAGES = 4
VMEM_LIMIT = 44 * 1024 * 1024
KEPT_ROOM = 6
BATCH = GROUP * UNROLL


def channel_chunks(width):
    lanes = LANES if width % LANES == 0 else width
    return [(start, lanes) for start in range(0, width, lanes)]


def plan_groups(cell_rows, cell_cols, live, row_tiles, col_bits):
    slots = cell_rows.shape[0]
    row_ids = jnp.arange(row_tiles, dtype=jnp.int32)
    slot_ids = jnp.arange(slots, dtype=jnp.int32)
    hits = (cell_rows[:, None] == row_ids[None, :]) & live[:, None]
    counts = jnp.sum(hits.astype(jnp.int32), axis=0)
    groups = (counts + (GROUP - 1)) // GROUP
    total = jnp.sum(groups)
    before = jnp.sum(jnp.where(row_ids[None, :] < cell_rows[:, None], groups[None, :], 0), axis=1)
    same = (cell_rows[:, None] == cell_rows[None, :]) & live[None, :] & (slot_ids[None, :] < slot_ids[:, None])
    rank = jnp.sum(same.astype(jnp.int32), axis=1)
    place = jnp.where(live, before * GROUP + rank, -1)
    room = -(-(slots + row_tiles * (GROUP - 1)) // BATCH) * BATCH
    seats = jnp.arange(room, dtype=jnp.int32)
    code = slot_ids * (1 << col_bits) + cell_cols + 1
    entries = jnp.sum(jnp.where(seats[:, None] == place[None, :], code[None, :], 0), axis=1) - 1
    ends = jnp.sum(jnp.where(row_ids[:, None] >= row_ids[None, :], groups[None, :], 0), axis=1)
    group_ids = jnp.arange(room // GROUP, dtype=jnp.int32)
    group_rows = jnp.sum((ends[None, :] <= group_ids[:, None]).astype(jnp.int32), axis=1)
    group_rows = jnp.minimum(group_rows, row_tiles - 1)
    closing = ends.reshape(lax.axis_size("col"), -1)[:, -1]
    last_turns = jnp.maximum((closing + (UNROLL - 1)) // UNROLL, 1) - 1
    return entries, group_rows, last_turns


def tile_kernel(*refs, lists, parts, begun, keep, col_bits, narrow, wide):
    plans = [refs[3 * k : 3 * k + 3] for k in range(lists)]
    place, picks = refs[3 * lists : 3 * lists + 2]
    refs = refs[3 * lists + 2 :]
    blocks = refs[: len(parts)]
    tiles = refs[len(parts)]
    started = refs[len(parts) + 1] if begun else None
    outs = refs[len(parts) + 1 + begun :][: narrow + wide + keep]
    sums, panel, ring, tile_sems, whole_sem, save_sems, *earlier = refs[len(parts) + 1 + begun + narrow + wide + keep :]
    block_tiles = blocks[0].shape[0]
    zero_seat = STAGES * BATCH
    spare = place[parts[0]] * block_tiles

    def fetch(entries, turn, seats=range(BATCH)):
        stage = lax.rem(turn, STAGES)
        for seat in seats:
            slot = lax.shift_right_logical(jnp.maximum(entries[turn * BATCH + seat], 0), col_bits)
            pltpu.make_async_copy(tiles.at[slot], ring.at[stage * BATCH + seat], tile_sems.at[stage]).start()

    def first_fetches(entries, count):
        lax.fori_loop(0, jnp.minimum(count, STAGES - 1), lambda turn, carry: fetch(entries, turn) or carry, 0)

    def save(number):
        piece = pl.ds(number * block_tiles, block_tiles)
        return pltpu.make_async_copy(sums.at[piece], outs[0].at[piece], save_sems.at[number])

    def step(ahead, entries, group_rows, turn, carry):
        stage = lax.rem(turn, STAGES)
        base = stage * BATCH
        pltpu.make_async_copy(
            tiles.at[pl.ds(0, BATCH)], ring.at[pl.ds(base, BATCH)], tile_sems.at[stage]
        ).wait()
        products = []
        for group in range(UNROLL):
            if ahead:
                fetch(entries, turn + ahead, range(group * GROUP, (group + 1) * GROUP))
            left, right = [], []
            for member in range(GROUP):
                seat = group * GROUP + member
                entry = entries[turn * BATCH + seat]
                left.append(ring[jnp.where(entry < 0, zero_seat, base + seat)])
                right.append(panel[jnp.where(entry < 0, spare, entry & ((1 << col_bits) - 1))])
            products.append(
                jnp.dot(
                    jnp.concatenate(left, axis=1),
                    jnp.concatenate(right, axis=0),
                    preferred_element_type=jnp.float32,
                )
            )
        for group in range(UNROLL):
            sums[group_rows[turn * UNROLL + group]] += products[group]
        if keep:
            for number in range(plans[0][2].shape[0]):
                pl.when(turn == plans[0][2][number])(save(number).start)
        return carry

    first_fetches(plans[0][0], plans[0][2][plans[0][2].shape[0] - 1] + 1)
    ring[zero_seat] = jnp.zeros(ring.shape[1:], ring.dtype)
    if begun:
        restore = pltpu.make_async_copy(started.at[pl.ds(0, sums.shape[0])], earlier[0], whole_sem)
        restore.start()
    sums[...] = jnp.zeros(sums.shape, sums.dtype)
    for number, part in enumerate(parts):
        panel[pl.ds(place[part] * block_tiles, block_tiles)] = blocks[number][...]
    for number, (entries, group_rows, turns) in enumerate(plans):
        count = turns[turns.shape[0] - 1] + 1
        if number:
            first_fetches(entries, count)
        steady = jnp.maximum(count - (STAGES - 1), 0)
        lax.fori_loop(0, steady, functools.partial(step, STAGES - 1, entries, group_rows), 0)
        lax.fori_loop(steady, count, functools.partial(step, 0, entries, group_rows), 0)

    if keep:
        for number in range(plans[0][2].shape[0]):
            save(number).wait()
        return
    if begun:
        restore.wait()
    for number, out in enumerate(outs):
        base = picks[number] * block_tiles

        def emit(tile, carry):
            value = sums[base + tile]
            if begun:
                value = value + earlier[0][base + tile]
            out[tile] = value.astype(out.dtype)
            return carry

        lax.fori_loop(0, block_tiles, emit, 0, unroll=4)


def tile_products(plans, place, picks, narrow, wide, blocks, cell_tiles, row_tiles, col_bits, begun=None, keep=False):
    parts = sorted(blocks)
    slots, tile_size, _ = cell_tiles.shape
    lanes = blocks[parts[0]].shape[-1]
    values = [blocks[part].reshape(-1, tile_size, lanes) for part in parts]
    block_tiles = values[0].shape[0]
    if keep:
        narrow = wide = 0
    smem = pl.BlockSpec(memory_space=pltpu.SMEM)
    vmem = pl.BlockSpec(memory_space=pltpu.VMEM)
    hbm = pl.BlockSpec(memory_space=pltpu.HBM)
    shape = (block_tiles, tile_size, lanes)
    total = jax.ShapeDtypeStruct((row_tiles, tile_size, lanes), jnp.float32)
    operands = [array for plan in plans for array in plan] + [place, picks] + values + [cell_tiles]
    in_specs = [smem] * (3 * len(plans) + 2) + [vmem] * len(values) + [hbm]
    if begun is not None:
        operands.append(begun)
        in_specs.append(hbm)
    sums = pltpu.VMEM(total.shape, total.dtype)
    scratch = [
        sums,
        pltpu.VMEM((1 << col_bits, tile_size, lanes), jnp.bfloat16),
        pltpu.VMEM((STAGES * BATCH + 1, tile_size, tile_size), jnp.bfloat16),
        pltpu.SemaphoreType.DMA((STAGES,)),
        pltpu.SemaphoreType.DMA(()),
        pltpu.SemaphoreType.DMA((row_tiles // block_tiles,)),
    ] + [sums] * (begun is not None)
    outs = pl.pallas_call(
        functools.partial(
            tile_kernel,
            lists=len(plans),
            parts=parts,
            begun=int(begun is not None),
            keep=int(keep),
            col_bits=col_bits,
            narrow=narrow,
            wide=wide,
        ),
        out_shape=[jax.ShapeDtypeStruct(shape, jnp.bfloat16)] * narrow
        + [jax.ShapeDtypeStruct(shape, jnp.float32)] * wide
        + [jax.ShapeDtypeStruct((KEPT_ROOM * row_tiles, tile_size, lanes), jnp.float32)] * keep,
        in_specs=in_specs,
        out_specs=[hbm if keep else vmem] * (narrow + wide + keep),
        scratch_shapes=scratch,
        compiler_params=pltpu.CompilerParams(vmem_limit_bytes=VMEM_LIMIT),
        cost_estimate=pl.CostEstimate(
            flops=slots * tile_size * tile_size * lanes,
            bytes_accessed=slots * tile_size * tile_size + row_tiles * tile_size * lanes,
            transcendentals=0,
        ),
        name="tile_products",
    )(*operands)
    if keep:
        return outs[0]
    return [out.reshape(block_tiles * tile_size, lanes) for out in outs[: narrow + wide]]


def swap(value, bits):
    size = lax.axis_size("row")
    return lax.ppermute(value, "row", [(i, i ^ bits) for i in range(size)])


def late_offset():
    size = lax.axis_size("row")
    return size - 2 if size > 2 and size & (size - 1) == 0 else None


def gather_far(piece):
    size = lax.axis_size("row")
    far = {0: piece}
    if size & (size - 1):
        for k in range(1, size):
            far[k] = lax.ppermute(piece, "row", [(i, (i - k) % size) for i in range(size)])
        return far
    for bits in range(2, size, 2):
        far[bits] = swap(piece, bits)
    return far


def gather_near(far):
    size = lax.axis_size("row")
    pieces = dict(far)
    if size > 1 and size & (size - 1) == 0:
        for bits, value in far.items():
            pieces[bits | 1] = swap(value, 1)
    return pieces


def gather_order():
    size = lax.axis_size("row")
    own = lax.axis_index("row")
    offsets = lax.broadcasted_iota(jnp.int32, (size,), 0)
    return lax.rem(own + offsets, size) if size & (size - 1) else own ^ offsets


def disjoint(pairs):
    return len({s for s, _ in pairs}) == len(pairs) and len({t for _, t in pairs}) == len(pairs)


def both_ways(ahead, up_pairs):
    size = lax.axis_size("col")
    own = lax.axis_index("col")
    down_pairs = [(size - 1 - s, size - 1 - t) for s, t in up_pairs]
    if disjoint(up_pairs + down_pairs):
        going_up = functools.reduce(jnp.logical_or, [own == s for s, _ in up_pairs])
        return [(jnp.where(going_up, own + ahead, own - ahead), up_pairs + down_pairs)]
    return [(own + ahead, up_pairs), (own - ahead, down_pairs)]


def line_messages():
    size = lax.axis_size("col")
    inner = size - 2
    hops = [both_ways(inner + 1 - turn, [(i, i + 1) for i in range(turn + 1)]) for turn in range(inner - 1)]
    near = []
    if size > 1:
        own = lax.axis_index("col")
        near = [(own + 1, [(i, i + 1) for i in range(size - 1)]), (own - 1, [(i + 1, i) for i in range(size - 1)])]
    far = both_ways(2, [(i, i + 2) for i in range(size - 2)]) if size > 2 else []
    return hops, near, far


def line_picks():
    hops, near, far = line_messages()
    first = hops[0] if hops else far
    later = [message for turn in hops[1:] for message in turn] + (far if hops else [])
    narrow = [index for index, _ in first + near]
    wide = [index for index, _ in later] + [lax.axis_index("col")]
    last = lax.axis_size("col") - 1
    numbers = lax.broadcasted_iota(jnp.int32, (len(narrow + wide),), 0)
    picks = jnp.zeros_like(numbers)
    for number, index in enumerate(narrow + wide):
        picks = jnp.where(numbers == number, jnp.clip(index, 0, last), picks)
    return picks, len(narrow), len(wide)


def reduce_line(picked):
    hops, near, far = line_messages()
    first = len(hops[0] if hops else far)
    sent = picked[:first]
    near_sent = picked[first : first + len(near)]
    later = list(picked[first + len(near) :])

    def move(values, messages):
        return [lax.ppermute(value, "col", pairs) for value, (_, pairs) in zip(values, messages)]

    def added(messages, carried):
        values = [later.pop(0) for _ in messages]
        carried = carried * (len(values) if len(carried) < len(values) else 1)
        if len(values) < len(carried):
            carried = carried[:1]
        return [(v + c.astype(jnp.float32)).astype(jnp.bfloat16) for v, c in zip(values, carried)]

    carried = None
    for turn in hops:
        values = sent if carried is None else added(turn, carried)
        carried = move(values, turn)
    parts = move(near_sent, near)
    if far:
        values = sent if carried is None else added(far, carried)
        parts = parts + move(values, far)
    return later[0], parts


def add_parts(own, parts):
    for part in parts:
        own = own + part.astype(jnp.float32)
    return own.astype(jnp.bfloat16)


def on_device(features, tiles, tile_rows, tile_cols, valid, weight, bias):
    sub_rows, width = features.shape
    tile_size = tiles.shape[3]
    row_tiles = sub_rows * lax.axis_size("col") // tile_size
    col_tiles = sub_rows * lax.axis_size("row") // tile_size
    col_bits = (col_tiles - 1).bit_length()
    chunks = channel_chunks(width)
    late = late_offset()
    cell_rows, cell_cols, live = tile_rows[0, 0], tile_cols[0, 0], valid[0, 0] > 0
    picks, narrow, wide = line_picks()
    place = gather_order()
    lives = [live]
    if late is not None:
        offset = (cell_cols // (sub_rows // tile_size)) ^ lax.axis_index("row")
        after = (offset | 1) == (late | 1)
        lives = [live & ~after, live & after]
    plans = [plan_groups(cell_rows, cell_cols, part, row_tiles, col_bits) for part in lives]
    far = []
    for start, size in chunks:
        far.append(gather_far(features[:, start : start + size]))
    products = functools.partial(
        tile_products, cell_tiles=tiles[0, 0], row_tiles=row_tiles, col_bits=col_bits, place=place, picks=picks
    )
    mixed = bias[None, :]
    for index, (start, size) in enumerate(chunks):
        begun, used = None, plans
        if index == 0 and late is not None:
            blocks = gather_near({bits: far[0][bits] for bits in far[0] if bits != late})
            begun = products(plans[:1], narrow=narrow, wide=wide, blocks=blocks, keep=True)
            used = plans[1:]
            far[0] = {late: far[0][late]}
        blocks = gather_near(far[index])
        picked = products(used, narrow=narrow, wide=wide, blocks=blocks, begun=begun)
        own, parts = reduce_line(picked)
        aggregated = add_parts(own, parts)
        mixed = mixed + jnp.dot(aggregated, weight[start : start + size], preferred_element_type=jnp.float32)
        if index < len(chunks) - 1:
            mixed = lax.optimization_barrier(mixed)
    return jnp.maximum(mixed, 0.0).astype(jnp.bfloat16)


def solution(mesh):
    def call(features, *operands):
        step = jax.shard_map(
            on_device,
            mesh=mesh,
            in_specs=(
                P(("row", "col"), None),
                P("row", "col", None, None, None),
                P("row", "col", None),
                P("row", "col", None),
                P("row", "col", None),
                P(),
                P(),
            ),
            out_specs=P(("row", "col"), None),
            check_vma=False,
        )
        return step(features, *operands)

    return call
```
